32 devices in a mesh: ep: 16 (over z, x, core), dp: 2 (over y).
Axes of the slice: x: 2, y: 2, z: 4, core: 2. Of those that a mesh axis runs over, the one named last changes fastest.
Arguments:
- tokens: bfloat16 [4096, 2048], P(('dp', 'ep')), parts along dimension 0, may hold values from -6 to 6
- expert_ids: int32 [4096, 8], P(('dp', 'ep')), parts along dimension 0, may hold values from 0 to 15, all different within a row; in each aligned block of 128 rows (0 to 127, 128 to 255, ...) at most 96 rows name the same one
- route_logits: float32 [4096, 8], P(('dp', 'ep')), parts along dimension 0, may hold values from -3 to 300
- w_gate: bfloat16 [16, 2048, 1024], P('ep'), may hold values from -0.125 to 0.125
- w_up: bfloat16 [16, 2048, 1024], P('ep'), may hold values from -0.125 to 0.125
- w_down: bfloat16 [16, 1024, 2048], P('ep'), may hold values from -0.1875 to 0.1875
Outputs:
- mixed_rows: bfloat16 [4096, 2048], P(('dp', 'ep')), parts along dimension 0
The draws below stay inside these ranges and needn't reach their ends.
There are 2 independent parts, one for each index of `dp`. The reference program is written for one: setup_inputs(seed, part) draws one part's arguments, and reference() takes and returns one part's arrays. A program takes and returns all parts, laid end to end along the dimension named above; an argument that names none is the same for every part. Nothing has to cross between parts.
Inputs may be any that keep to these rules, and one draw needn't show every extreme that they name: `expert_ids`: each row names 8 different experts; among the 128 rows of one device no expert is named more than 96 times, a bound that some block reaches.
All inputs are finite; a program needn't handle non-finite values.
Results may differ from the reference program's by a relative error of at most 0.0058.
Values may be sent and summed in bfloat16 or wider, within the bound.
A program may use at most 128 MiB of HBM per device.

```python
import math
import jax
import jax.numpy as jnp
import numpy as np
from jax import lax

D = 2048
FF = 1024
TOP = 8
TOK_DEV = 128
EXPERTS = 16
TOKENS = 2048
CAP = 96
N_EP = 16


def draw_route_logits(key, part):
    first_key = jax.random.fold_in(key, 11)
    values = jnp.clip(jax.random.normal(first_key, (TOKENS, TOP), jnp.float32) * 0.4, -0.75, 0.75)
    return values


def block_scale(key, extent, shards, smallest, top_value):
    loudness, own = 1.0, jax.random.fold_in(key, 6)
    for dim, shards_of in shards:
        steps = jnp.exp(jax.random.uniform(jax.random.fold_in(own, dim), (shards_of,), jnp.float32, smallest / len(shards), top_value / len(shards)))
        loudness = loudness * jnp.repeat(steps, extent[dim] // shards_of).reshape([-1 if axis == dim else 1 for axis in range(len(extent))])
    return loudness


def shared_out(stream_key, own, number, rows, number_of, top, bound, skew):
    ranking = jax.random.permutation(stream_key, number_of)
    packed, ordinary = shares(number_of, rows * top, bound, skew, True), shares(number_of, rows * top, bound, skew, False)
    places = jnp.arange(number_of)

    def named(sizes, turn):
        used = int((sizes > 0).sum())
        fixed = max(1, used // 4)
        moved = fixed + (places - fixed + turn * (used - fixed)) % max(1, number_of - fixed)
        return jnp.zeros((number_of,), jnp.int32).at[ranking[jnp.where(places < fixed, places, moved)]].set(jnp.asarray(sizes, jnp.int32))

    sizes = jnp.where(number % 4 == 0, named(packed, number // 4), named(ordinary, number - number // 4 - 1))
    mixed = jax.random.permutation(jax.random.fold_in(own, 3), number_of)
    source_of, sink = mixed[0:number_of // 2 * 2:2], mixed[1:number_of // 2 * 2:2]
    slack = jnp.minimum(sizes[source_of] - 1, bound - sizes[sink]) // 2
    slack = jnp.where((source_of == ranking[0]) | (sink == ranking[0]) | (sizes[sink] == 0), 0, jnp.maximum(slack, 0))
    moved = jax.random.randint(jax.random.fold_in(own, 4), (number_of // 2,), 0, 1 << 20) % (slack + 1)
    sizes = sizes.at[source_of].add(-moved).at[sink].add(moved)
    members = jnp.searchsorted(jnp.cumsum(sizes), jnp.arange(rows * top), side="right").astype(jnp.int32)
    grid = members.reshape(top, rows).T
    grid = grid[jax.random.permutation(jax.random.fold_in(own, 1), rows)]
    turn = jax.random.randint(jax.random.fold_in(own, 2), (rows, 1), 0, top)
    return jnp.take_along_axis(grid, (jnp.arange(top)[None, :] + turn) % top, axis=1)


def shares(count, total, bound, skew, full):
    loads = [(1 << 20) // math.isqrt(grade ** skew) + 1 for grade in range(1, count + 1)]
    largest = bound if full else min(bound, max(-(-total // count), total * loads[0] // sum(loads)))
    least = 1 if total - largest >= count - 1 else 0
    given, rest = [largest] + [least] * (count - 1), total - largest - least * (count - 1)
    while rest > 0:
        movable = [i for i in range(1, count) if given[i] < largest] or [i for i in range(1, count) if given[i] < bound]
        pool, left = sum([loads[i] for i in movable]), rest
        for i in movable:
            more = min(bound - given[i], max(1, left * loads[i] // pool), rest)
            given[i] = given[i] + more
            rest = rest - more
    return np.array(given)


def centred(own_key, extent, scale, bound, pieces=(), kind=jnp.bfloat16):
    values = jax.random.normal(own_key, extent, jnp.float32) * scale
    if len(pieces) > 0:
        values = block_scale(own_key, extent, pieces, -0.22, 0.18) * values
    return jnp.clip(values, min=-bound, max=bound).astype(kind)


def setup_inputs(seed: int = 0, part: int = 0) -> dict:
    key_list = jax.random.split(jax.random.key(seed), 7)
    part_keys = jax.random.split(jax.random.fold_in(key_list[6], part), 7)
    tokens = centred(part_keys[0], (TOKENS, D), 1.0, 6.0, ((0, 16),))
    expert_ids_keys = jax.random.split(jax.random.fold_in(part_keys[1], 1), TOKENS // TOK_DEV)
    expert_ids_turns = jax.random.permutation(jax.random.fold_in(part_keys[1], 3), TOKENS // TOK_DEV)
    expert_ids = jax.vmap(lambda own, number: shared_out(jax.random.fold_in(part_keys[1], 2), own, number, TOK_DEV, EXPERTS, TOP, CAP, 2))(expert_ids_keys, expert_ids_turns).reshape((TOKENS, TOP))
    route_logits = draw_route_logits(jax.random.fold_in(jax.random.fold_in(key_list[6], part), 71), part)
    w_gate = centred(key_list[3], (EXPERTS, D, FF), D ** -0.5, 0.125, ((0, 16),))
    w_up = centred(key_list[4], (EXPERTS, D, FF), D ** -0.5, 0.125, ((0, 16),))
    w_down = centred(key_list[5], (EXPERTS, FF, D), FF ** -0.5, 0.1875, ((0, 16),))
    return {"tokens": tokens, "expert_ids": expert_ids, "route_logits": route_logits, "w_gate": w_gate, "w_up": w_up, "w_down": w_down}


def expert_ffn(rows, gate_weight, up_weight, down_weight):
    gate = jnp.dot(rows, gate_weight, preferred_element_type=jnp.float32)
    up_part = jnp.dot(rows, up_weight, preferred_element_type=jnp.float32)
    hidden = (jax.nn.silu(gate) * up_part).astype(jnp.bfloat16)
    return jnp.dot(hidden, down_weight, preferred_element_type=jnp.float32).astype(jnp.bfloat16)


def reference(tokens, expert_ids, route_logits, w_gate, w_up, w_down):
    token_count, model_width = tokens.shape
    picks = expert_ids.shape[1]
    gates = jax.nn.softmax(route_logits.astype(jnp.float32), axis=-1)
    flat_ids = expert_ids.reshape(-1)
    flat_gates = gates.reshape(-1)
    flat_token = (jnp.arange(token_count * picks, dtype=jnp.int32) // picks).astype(jnp.int32)
    buffer = N_EP * CAP
    padded = jnp.concatenate([tokens, jnp.zeros((1, model_width), tokens.dtype)], 0)

    def expert_pass(mixed, inputs):
        gate_weight, up_weight, down_weight, expert = inputs
        chosen = flat_ids == expert
        place = (jnp.cumsum(chosen.astype(jnp.int32)) - 1).astype(jnp.int32)
        target = jnp.where(chosen, place, buffer).astype(jnp.int32)
        rows_token = jnp.full((buffer,), token_count, jnp.int32).at[target].set(flat_token, mode="drop")
        rows_gate = jnp.zeros((buffer,), jnp.float32).at[target].set(flat_gates, mode="drop")
        answer = expert_ffn(padded[rows_token], gate_weight, up_weight, down_weight)
        mixed = mixed.at[rows_token].add(rows_gate[:, None] * answer.astype(jnp.float32), mode="drop")
        return mixed, None

    start = jnp.zeros((token_count, model_width), jnp.float32)
    mixed, _ = lax.scan(expert_pass, start, (w_gate, w_up, w_down, jnp.arange(EXPERTS, dtype=jnp.int32)))
    return mixed.astype(jnp.bfloat16)
```

```python
import functools

import jax
import jax.numpy as jnp
from jax import lax
from jax.experimental import pallas as pl
from jax.experimental.pallas import tpu as pltpu
from jax.sharding import PartitionSpec as P

VMEM_BYTES = 63 * 1024 * 1024


def expert_ffn(rows, gate_weight, up_weight, down_weight):
    gate = jnp.dot(rows, gate_weight, preferred_element_type=jnp.float32)
    up_part = jnp.dot(rows, up_weight, preferred_element_type=jnp.float32)
    hidden = (jax.nn.silu(gate) * up_part).astype(jnp.bfloat16)
    return jnp.dot(hidden, down_weight, preferred_element_type=jnp.float32).astype(jnp.bfloat16)


def blockwise(rows, live_rows, weights):
    turns = (live_rows + 127) // 128

    def step(block_index, result):
        first_row = block_index * 128
        block_rows = lax.dynamic_slice_in_dim(rows, first_row, 128, 0)
        answer = expert_ffn(block_rows, weights[0], weights[1], weights[2])
        return lax.dynamic_update_slice_in_dim(result, answer, first_row, 0)

    return lax.fori_loop(jnp.int32(0), turns, step, jnp.zeros(rows.shape, jnp.bfloat16))


def per_device(tokens, expert_ids, route_logits, w_gate, w_up, w_down):
    tok_rows, model_width = tokens.shape
    picks = expert_ids.shape[1]
    experts = lax.axis_size("ep")
    capacity = min(tok_rows, 3 * tok_rows * picks // (2 * experts))
    row_quota = tok_rows * picks
    received = experts * capacity
    spill_count = (max(received - row_quota, 128) + 127) // 128 * 128
    length = row_quota + spill_count
    flat_ids = expert_ids.reshape(-1)
    one_hot = (flat_ids[:, None] == jnp.arange(experts, dtype=jnp.int32)[None, :]).astype(jnp.int32)
    earlier = jnp.cumsum(one_hot, axis=0) - one_hot
    slot_rank = jnp.sum(earlier * one_hot, axis=1)
    counts = jnp.sum(one_hot, axis=0)
    slot_place = flat_ids * capacity + slot_rank
    source_row = jnp.arange(row_quota, dtype=jnp.int32) // picks
    slot_token = jnp.full((received,), tok_rows, jnp.int32).at[slot_place].set(source_row)
    padded_tokens = jnp.concatenate([tokens, jnp.zeros((1, model_width), tokens.dtype)], 0)
    outgoing = padded_tokens[slot_token].reshape(experts, capacity, model_width)
    all_counts = lax.all_gather(counts, "ep", axis=0, tiled=True).reshape(experts, experts)
    own_index = lax.axis_index("ep")
    from_sources = lax.dynamic_index_in_dim(all_counts, own_index, 1, keepdims=False)
    incoming = lax.all_to_all(outgoing, "ep", split_axis=0, concat_axis=0, tiled=True)
    offsets = jnp.cumsum(from_sources) - from_sources
    live_rows = jnp.sum(from_sources)
    slot_numbers = jnp.arange(capacity, dtype=jnp.int32)
    live_slot = slot_numbers[None, :] < from_sources[:, None]
    position = jnp.where(live_slot, offsets[:, None] + slot_numbers[None, :], length).reshape(-1)
    gather_order = (
        jnp.full((length,), received, jnp.int32)
        .at[position]
        .set(jnp.arange(received, dtype=jnp.int32), mode="drop")
    )
    flat_incoming = jnp.concatenate(
        [incoming.reshape(received, model_width), jnp.zeros((1, model_width), jnp.bfloat16)], 0
    )
    packed = flat_incoming[gather_order]
    own_weights = (w_gate[0], w_up[0], w_down[0])
    results = blockwise(packed, live_rows, own_weights)
    results_ext = jnp.concatenate([results, jnp.zeros((1, model_width), jnp.bfloat16)], 0)
    outgoing_back = results_ext[position].reshape(experts, capacity, model_width)
    answers = lax.all_to_all(outgoing_back, "ep", split_axis=0, concat_axis=0, tiled=True)
    mix_weights = jax.nn.softmax(route_logits, axis=-1)
    picked = answers.reshape(received, model_width)[slot_place].reshape(
        tok_rows, picks, model_width
    )
    mixed_rows = jnp.zeros((tok_rows, model_width), jnp.float32)
    for column in range(picks):
        mixed_rows = mixed_rows + mix_weights[:, column : column + 1] * picked[:, column].astype(
            jnp.float32
        )
    return mixed_rows.astype(jnp.bfloat16)


def ring_place(chip, ring):
    column, row = chip % 2, chip // 2
    return row + column * (ring - 1 - 2 * row)


def chip_at(place, ring):
    column = place // (ring // 2)
    return 2 * (place + column * (ring - 1 - 2 * place)) + column


def remote(src, dst, send_sem, recv_sem, target):
    return pltpu.make_async_remote_copy(
        src_ref=src,
        dst_ref=dst,
        send_sem=send_sem,
        recv_sem=recv_sem,
        device_id={"ep": target},
        device_id_type=pl.DeviceIdType.MESH,
    )


def fused_kernel(
    n,
    tok_ref,
    ids_ref,
    logits_ref,
    wg_hbm,
    wu_hbm,
    wd_hbm,
    out_ref,
    xs,
    wg,
    wu,
    wd,
    ps,
    sib,
    got_r,
    got_l,
    put_r,
    put_l,
    hid,
    gate_rows,
    gate_all,
    gate_col,
    load_sem,
    gate_send,
    gate_recv,
    ag_send,
    ag_recv,
    pass_send,
    pass_recv,
    own_sem,
    sib_send,
    sib_recv,
    rs_send,
    rs_recv,
):
    ring = n // 2
    far = ring // 2
    chunks = ring - 1
    tok_rows, width = tok_ref.shape
    part = tok_rows // 2
    ff = wg.shape[1]
    picks = ids_ref.shape[1]
    me = lax.axis_index("ep")
    core, chip = me % 2, me // 2
    other = 1 - core
    place = ring_place(chip, ring)
    right = chip_at((place + 1) % ring, ring) * 2 + core
    left = chip_at((place + ring - 1) % ring, ring) * 2 + core
    twin = chip * 2 + other

    barrier = pltpu.get_barrier_semaphore()

    def greet(step, carry):
        pl.semaphore_signal(
            barrier,
            inc=1,
            device_id={"ep": (me + step) % n},
            device_id_type=pl.DeviceIdType.MESH,
        )
        return carry

    lax.fori_loop(1, n, greet, 0)

    own_load = pltpu.make_async_copy(tok_ref, xs.at[0, core], load_sem.at[0])
    own_load.start()
    weight_loads = [
        pltpu.make_async_copy(wg_hbm.at[0], wg, load_sem.at[1]),
        pltpu.make_async_copy(wu_hbm.at[0], wu, load_sem.at[2]),
        pltpu.make_async_copy(wd_hbm.at[0], wd, load_sem.at[3]),
    ]

    logits = logits_ref[...]
    powers = jnp.exp(logits - jnp.max(logits, axis=1, keepdims=True))
    gates = powers / jnp.sum(powers, axis=1, keepdims=True)
    ids = ids_ref[...]
    lanes = lax.broadcasted_iota(jnp.int32, (tok_rows, 128), 1)
    spread = jnp.zeros((tok_rows, 128), jnp.float32)
    for pick in range(picks):
        spread = spread + jnp.where(
            ids[:, pick : pick + 1] == lanes, gates[:, pick : pick + 1], 0.0
        )
    turned = spread.T
    for expert in range(n):
        gate_rows[expert] = turned[expert : expert + 1, :]
    gate_all[0] = gate_rows[me]

    own_load.wait()
    pl.semaphore_wait(barrier, n - 1)

    def ag_copy(way, s):
        hop = s // 2
        lane, sign, target = (s % 2, -1, right) if way == 0 else (1 - s % 2, 1, left)
        rows = pl.ds(lane * part, part)
        return remote(
            xs.at[(sign * hop) % ring, core, rows],
            xs.at[(sign * (hop + 1)) % ring, core, rows],
            ag_send.at[way, s],
            ag_recv.at[way, s],
            target,
        )

    def pass_copy(way, s, whose):
        lane, sign = (s % 2, -1) if way == 0 else (1 - s % 2, 1)
        ref = xs.at[(sign * (s // 2 + 1)) % ring, whose, pl.ds(lane * part, part)]
        return remote(ref, ref, pass_send.at[way, s], pass_recv.at[way, s], twin)

    def own_copy(whose):
        ref = xs.at[0, whose]
        return remote(ref, ref, own_sem.at[0], own_sem.at[1], twin)

    def gate_copy(step):
        target = (me + step) % n
        return remote(
            gate_rows.at[target],
            gate_all.at[step],
            gate_send.at[step],
            gate_recv.at[step],
            target,
        )

    for s in range(2):
        for way in range(2):
            ag_copy(way, s).start()
    own_copy(core).start()
    for load in weight_loads:
        load.start()

    def send_gate(step, carry):
        gate_copy(step).start()
        return carry

    lax.fori_loop(1, n, send_gate, 0)

    def ag_event(k):
        for way in range(2):
            ag_copy(way, k).wait_recv()
            if k + 2 < chunks:
                ag_copy(way, k + 2).start()
            pass_copy(way, k, core).start()

    def sib_copy(o, whose):
        return remote(
            ps.at[o % ring, whose],
            sib.at[o % ring],
            sib_send.at[o % ring],
            sib_recv.at[o % ring],
            twin,
        )

    def rs_copy(way, s):
        put, got, target = (put_r, got_r, right) if way == 0 else (put_l, got_l, left)
        return remote(
            put.at[s], got.at[s], rs_send.at[way, s], rs_recv.at[way, s], target
        )

    joined = set()

    def join(o):
        if o % ring not in joined:
            joined.add(o % ring)
            sib_copy(o, core).wait_recv()

    def chip_sum(o, rows):
        return ps[o % ring, core, rows, :].astype(jnp.float32) + sib[
            o % ring, rows, :
        ].astype(jnp.float32)

    def rs_event(way, s):
        o = far if s == 0 else far - (s + 1) // 2
        lane, o = (s % 2, o) if way == 0 else (1 - s % 2, -o)
        join(o)
        put, got = (put_r, got_r) if way == 0 else (put_l, got_l)
        total = chip_sum(o, pl.ds(lane * part, part))
        if s >= 2:
            rs_copy(way, s - 2).wait_recv()
            total = total + got[s - 2].astype(jnp.float32)
        put[s] = total.astype(jnp.bfloat16)
        rs_copy(way, s).start()

    def arrive(o):
        if o == 0:
            own_copy(other).wait_recv()
        elif o == far:
            pass_copy(0, chunks - 1, other).wait_recv()
            pass_copy(1, chunks - 1, other).wait_recv()
        else:
            for s in (2 * abs(o) - 2, 2 * abs(o) - 1):
                pass_copy(0 if o < 0 else 1, s, other).wait_recv()

    ff_tile = ff // 4
    out_tile = width // 4

    def hidden_part(slot, first, last):
        def body(j, carry):
            x = xs[slot].reshape(2 * tok_rows, width)
            cols = pl.ds(pl.multiple_of(j * ff_tile, ff_tile), ff_tile)
            gate = jnp.dot(x, wg[:, cols], preferred_element_type=jnp.float32)
            up = jnp.dot(x, wu[:, cols], preferred_element_type=jnp.float32)
            hid[:, cols] = (gate / (1.0 + jnp.exp(-gate)) * up).astype(jnp.bfloat16)
            return carry

        lax.fori_loop(first, last, body, 0)

    def answer_part(slot):
        def body(j, carry):
            cols = pl.ds(pl.multiple_of(j * out_tile, out_tile), out_tile)
            answer = jnp.dot(hid[...], wd[:, cols], preferred_element_type=jnp.float32)
            scale = jnp.concatenate([gate_col[...]] * (out_tile // 128), axis=1)
            ps[slot, :, :, cols] = (
                (answer * scale).astype(jnp.bfloat16).reshape(2, tok_rows, out_tile)
            )
            return carry

        lax.fori_loop(0, 4, body, 0)

    order = [0]
    for d in range(1, far - 1):
        order += [-d, d]
    order = order[:-1] + [1 - far, far, far - 1, far - 2]
    hooks = {}
    for k in range(chunks):
        b = k // 2 + 1
        step = min(order.index(-b) if b < far else ring, order.index(b))
        hooks.setdefault(min(3 * step - 1, max(1, 7 * k // 3)), []).append(
            functools.partial(ag_event, k)
        )
    last = 3 * ring
    hooks.setdefault(last - 6, []).extend(
        [functools.partial(rs_event, w, s) for w, s in ((0, 0), (1, 0), (1, 1))]
    )
    hooks.setdefault(last - 3, []).append(functools.partial(rs_event, 0, 1))
    hooks.setdefault(last - 2, []).extend(
        [functools.partial(rs_event, w, 2) for w in (1, 0)]
    )

    def wait_gate(step, carry):
        gate_copy(step).wait_recv()
        return carry

    third = 0
    for index, o in enumerate(order):
        slot = o % ring
        arrive(o)
        if index == 0:
            weight_loads[0].wait()
            weight_loads[1].wait()
        for piece in range(3):
            if piece == 0:
                hidden_part(slot, 0, 2)
            elif piece == 1:
                hidden_part(slot, 2, 4)
            else:
                if index == 0:
                    weight_loads[2].wait()
                    lax.fori_loop(1, n, wait_gate, 0)
                for whose in range(2):
                    source = chip_at((place + slot) % ring, ring) * 2 + whose
                    row = gate_all[(me + n - source) % n]
                    gate_col[pl.ds(whose * tok_rows, tok_rows), :] = jnp.broadcast_to(
                        row, (128, tok_rows)
                    ).T
                answer_part(slot)
                sib_copy(o, other).start()
            for hook in hooks.get(third, []):
                hook()
            third += 1

    for s in range(3, chunks):
        for way in (1, 0):
            rs_event(way, s)
    join(0)
    for lane in (1, 0):
        rows = pl.ds(lane * part, part)
        s_right, s_left = (chunks - 2, chunks - 1) if lane == 1 else (chunks - 1, chunks - 2)
        if lane == 1:
            for s in (chunks - 2, chunks - 1):
                for way in range(2):
                    rs_copy(way, s).wait_recv()
        total = chip_sum(0, rows)
        total = total + got_r[s_right].astype(jnp.float32)
        total = total + got_l[s_left].astype(jnp.float32)
        out_ref[rows, :] = total.astype(jnp.bfloat16)
    for s in range(chunks):
        for way in range(2):
            ag_copy(way, s).wait_send()
            pass_copy(way, s, core).wait_send()
            rs_copy(way, s).wait_send()
    for o in range(ring):
        join(o)
        sib_copy(o, other).wait_send()
    own_copy(core).wait_send()

    def drain_gate(step, carry):
        gate_copy(step).wait_send()
        return carry

    lax.fori_loop(1, n, drain_gate, 0)


def fused_scratch(n, tok_rows, width, ff):
    ring = n // 2
    chunks, part, bf16 = ring - 1, tok_rows // 2, jnp.bfloat16
    buffers = [
        ((ring, 2, tok_rows, width), bf16),
        ((width, ff), bf16),
        ((width, ff), bf16),
        ((ff, width), bf16),
        ((ring, 2, tok_rows, width), bf16),
        ((ring, tok_rows, width), bf16),
        ((chunks, part, width), bf16),
        ((chunks, part, width), bf16),
        ((chunks, part, width), bf16),
        ((chunks, part, width), bf16),
        ((2 * tok_rows, ff), bf16),
        ((n, 1, tok_rows), jnp.float32),
        ((n, 1, tok_rows), jnp.float32),
        ((2 * tok_rows, 128), jnp.float32),
    ]
    sems = [(4,), (n,), (n,), (2, chunks), (2, chunks), (2, chunks), (2, chunks), (2,), (ring,), (ring,), (2, chunks), (2, chunks)]
    size = 0
    for shape, kind in buffers:
        count = jnp.dtype(kind).itemsize
        for extent in shape:
            count = count * extent
        size = size + count
    scratch = [pltpu.VMEM(shape, kind) for shape, kind in buffers]
    return scratch + [pltpu.SemaphoreType.DMA(shape) for shape in sems], size


def fused_device(tokens, expert_ids, route_logits, w_gate, w_up, w_down):
    n = lax.axis_size("ep")
    tok_rows, width = tokens.shape
    ff = w_gate.shape[2]
    scratch, size = fused_scratch(n, tok_rows, width, ff)
    anywhere, vmem = pl.BlockSpec(memory_space=pl.ANY), pl.BlockSpec(memory_space=pltpu.VMEM)
    return pl.pallas_call(
        functools.partial(fused_kernel, n),
        out_shape=jax.ShapeDtypeStruct((tok_rows, width), jnp.bfloat16),
        in_specs=[anywhere, vmem, vmem, anywhere, anywhere, anywhere],
        out_specs=vmem,
        scratch_shapes=scratch,
        compiler_params=pltpu.CompilerParams(
            collective_id=0, has_side_effects=True, vmem_limit_bytes=VMEM_BYTES
        ),
    )(tokens, expert_ids, route_logits, w_gate, w_up, w_down)


def layer(tokens, expert_ids, route_logits, w_gate, w_up, w_down):
    n = lax.axis_size("ep")
    tok_rows, width = tokens.shape
    ff = w_gate.shape[2]
    size = fused_scratch(n, tok_rows, width, ff)[1]
    fits = size + 8 * tok_rows * width < VMEM_BYTES
    if fits and n % 4 == 0 and n >= 12 and tok_rows == 128 and n <= 128:
        return fused_device(tokens, expert_ids, route_logits, w_gate, w_up, w_down)
    return per_device(tokens, expert_ids, route_logits, w_gate, w_up, w_down)


def solution(mesh):
    in_specs = (
        P(("dp", "ep"), None),
        P(("dp", "ep"), None),
        P(("dp", "ep"), None),
        P("ep", None, None),
        P("ep", None, None),
        P("ep", None, None),
    )
    out_specs = P(("dp", "ep"), None)
    return jax.shard_map(
        layer, mesh=mesh, in_specs=in_specs, out_specs=out_specs, check_vma=False
    )
```

```python
import functools

import jax
import jax.numpy as jnp
from jax import lax
from jax.experimental import pallas as pl
from jax.experimental.pallas import tpu as pltpu
from jax.sharding import PartitionSpec as P

VMEM_BYTES = 63 * 1024 * 1024


def expert_ffn(rows, gate_weight, up_weight, down_weight):
    gate = jnp.dot(rows, gate_weight, preferred_element_type=jnp.float32)
    up_part = jnp.dot(rows, up_weight, preferred_element_type=jnp.float32)
    hidden = (jax.nn.silu(gate) * up_part).astype(jnp.bfloat16)
    return jnp.dot(hidden, down_weight, preferred_element_type=jnp.float32).astype(jnp.bfloat16)


def blockwise(rows, live_rows, weights):
    turns = (live_rows + 127) // 128

    def step(block_index, result):
        first_row = block_index * 128
        block_rows = lax.dynamic_slice_in_dim(rows, first_row, 128, 0)
        answer = expert_ffn(block_rows, weights[0], weights[1], weights[2])
        return lax.dynamic_update_slice_in_dim(result, answer, first_row, 0)

    return lax.fori_loop(jnp.int32(0), turns, step, jnp.zeros(rows.shape, jnp.bfloat16))


def per_device(tokens, expert_ids, route_logits, w_gate, w_up, w_down):
    tok_rows, model_width = tokens.shape
    picks = expert_ids.shape[1]
    experts = lax.axis_size("ep")
    capacity = min(tok_rows, 3 * tok_rows * picks // (2 * experts))
    row_quota = tok_rows * picks
    received = experts * capacity
    spill_count = (max(received - row_quota, 128) + 127) // 128 * 128
    length = row_quota + spill_count
    flat_ids = expert_ids.reshape(-1)
    one_hot = (flat_ids[:, None] == jnp.arange(experts, dtype=jnp.int32)[None, :]).astype(jnp.int32)
    earlier = jnp.cumsum(one_hot, axis=0) - one_hot
    slot_rank = jnp.sum(earlier * one_hot, axis=1)
    counts = jnp.sum(one_hot, axis=0)
    slot_place = flat_ids * capacity + slot_rank
    source_row = jnp.arange(row_quota, dtype=jnp.int32) // picks
    slot_token = jnp.full((received,), tok_rows, jnp.int32).at[slot_place].set(source_row)
    padded_tokens = jnp.concatenate([tokens, jnp.zeros((1, model_width), tokens.dtype)], 0)
    outgoing = padded_tokens[slot_token].reshape(experts, capacity, model_width)
    all_counts = lax.all_gather(counts, "ep", axis=0, tiled=True).reshape(experts, experts)
    own_index = lax.axis_index("ep")
    from_sources = lax.dynamic_index_in_dim(all_counts, own_index, 1, keepdims=False)
    incoming = lax.all_to_all(outgoing, "ep", split_axis=0, concat_axis=0, tiled=True)
    offsets = jnp.cumsum(from_sources) - from_sources
    live_rows = jnp.sum(from_sources)
    slot_numbers = jnp.arange(capacity, dtype=jnp.int32)
    live_slot = slot_numbers[None, :] < from_sources[:, None]
    position = jnp.where(live_slot, offsets[:, None] + slot_numbers[None, :], length).reshape(-1)
    gather_order = (
        jnp.full((length,), received, jnp.int32)
        .at[position]
        .set(jnp.arange(received, dtype=jnp.int32), mode="drop")
    )
    flat_incoming = jnp.concatenate(
        [incoming.reshape(received, model_width), jnp.zeros((1, model_width), jnp.bfloat16)], 0
    )
    packed = flat_incoming[gather_order]
    own_weights = (w_gate[0], w_up[0], w_down[0])
    results = blockwise(packed, live_rows, own_weights)
    results_ext = jnp.concatenate([results, jnp.zeros((1, model_width), jnp.bfloat16)], 0)
    outgoing_back = results_ext[position].reshape(experts, capacity, model_width)
    answers = lax.all_to_all(outgoing_back, "ep", split_axis=0, concat_axis=0, tiled=True)
    mix_weights = jax.nn.softmax(route_logits, axis=-1)
    picked = answers.reshape(received, model_width)[slot_place].reshape(
        tok_rows, picks, model_width
    )
    mixed_rows = jnp.zeros((tok_rows, model_width), jnp.float32)
    for column in range(picks):
        mixed_rows = mixed_rows + mix_weights[:, column : column + 1] * picked[:, column].astype(
            jnp.float32
        )
    return mixed_rows.astype(jnp.bfloat16)


def ring_place(chip, ring):
    column, row = chip % 2, chip // 2
    return row + column * (ring - 1 - 2 * row)


def chip_at(place, ring):
    column = place // (ring // 2)
    return 2 * (place + column * (ring - 1 - 2 * place)) + column


def remote(src, dst, send_sem, recv_sem, target):
    return pltpu.make_async_remote_copy(
        src_ref=src,
        dst_ref=dst,
        send_sem=send_sem,
        recv_sem=recv_sem,
        device_id={"ep": target},
        device_id_type=pl.DeviceIdType.MESH,
    )


def fused_kernel(
    n,
    tok_ref,
    ids_ref,
    logits_ref,
    wg_hbm,
    wu_hbm,
    wd_hbm,
    out_ref,
    xs,
    wg,
    wu,
    wd,
    ps,
    sib,
    got_r,
    got_l,
    put_r,
    put_l,
    hid,
    gate_rows,
    gate_all,
    gate_col,
    load_sem,
    gate_send,
    gate_recv,
    ag_send,
    ag_recv,
    pass_send,
    pass_recv,
    own_sem,
    sib_send,
    sib_recv,
    rs_send,
    rs_recv,
):
    ring = n // 2
    chunks = ring - 1
    tok_rows, width = tok_ref.shape
    part = tok_rows // 2
    ff = wg.shape[1]
    me = lax.axis_index("ep")
    core, chip = me % 2, me // 2
    other = 1 - core
    place = ring_place(chip, ring)
    right = chip_at((place + 1) % ring, ring) * 2 + core
    left = chip_at((place + ring - 1) % ring, ring) * 2 + core
    twin = chip * 2 + other

    barrier = pltpu.get_barrier_semaphore()

    def greet(step, carry):
        pl.semaphore_signal(
            barrier,
            inc=1,
            device_id={"ep": (me + step) % n},
            device_id_type=pl.DeviceIdType.MESH,
        )
        return carry

    lax.fori_loop(1, n, greet, 0)

    own_load = pltpu.make_async_copy(tok_ref, xs.at[0, core], load_sem.at[0])
    own_load.start()
    weight_loads = [
        pltpu.make_async_copy(wg_hbm.at[0], wg, load_sem.at[1]),
        pltpu.make_async_copy(wu_hbm.at[0], wu, load_sem.at[2]),
        pltpu.make_async_copy(wd_hbm.at[0], wd, load_sem.at[3]),
    ]

    logits = logits_ref[...]
    powers = jnp.exp(logits - jnp.max(logits, axis=0, keepdims=True))
    gates = powers / jnp.sum(powers, axis=0, keepdims=True)
    ids = ids_ref[...]
    for expert in range(n):
        gate_rows[expert] = jnp.sum(
            jnp.where(ids == expert, gates, 0.0), axis=0, keepdims=True
        )
    gate_all[0] = gate_rows[me]

    own_load.wait()
    pl.semaphore_wait(barrier, n - 1)

    def ag_copy(way, s):
        target = right if way == 0 else left
        rows = pl.ds(way * part, part)
        if s < 2:
            lane = s if way == 0 else 1 - s
            src = xs.at[0, core, pl.ds(lane * part, part)]
        else:
            src = xs.at[s - 1, core, rows]
        return remote(
            src, xs.at[s + 1, core, rows], ag_send.at[way, s], ag_recv.at[way, s], target
        )

    def pass_copy(way, s, whose):
        ref = xs.at[s + 1, whose, pl.ds(way * part, part)]
        return remote(ref, ref, pass_send.at[way, s], pass_recv.at[way, s], twin)

    def own_copy(whose):
        ref = xs.at[0, whose]
        return remote(ref, ref, own_sem.at[0], own_sem.at[1], twin)

    def gate_copy(step):
        target = (me + step) % n
        return remote(
            gate_rows.at[target],
            gate_all.at[step],
            gate_send.at[step],
            gate_recv.at[step],
            target,
        )

    for s in range(2):
        for way in range(2):
            ag_copy(way, s).start()
    own_copy(core).start()
    for load in weight_loads:
        load.start()

    def send_gate(step, carry):
        gate_copy(step).start()
        return carry

    lax.fori_loop(1, n, send_gate, 0)

    def ag_event(k):
        for way in range(2):
            ag_copy(way, k).wait_recv()
            if k + 2 < chunks:
                ag_copy(way, k + 2).start()
            pass_copy(way, k, core).start()

    def sib_copy(slot, whose):
        return remote(
            ps.at[slot, whose], sib.at[slot], sib_send.at[slot], sib_recv.at[slot], twin
        )

    def rs_copy(way, k):
        put, got, target = (put_r, got_r, right) if way == 0 else (put_l, got_l, left)
        return remote(
            put.at[k], got.at[k], rs_send.at[way, k], rs_recv.at[way, k], target
        )

    def chip_sum(slot, rows):
        return ps[slot, core, rows, :].astype(jnp.float32) + sib[slot, rows, :].astype(
            jnp.float32
        )

    def rs_event(k):
        sib_copy(k + 1, core).wait_recv()
        for way in range(2):
            put, got = (put_r, got_r) if way == 0 else (put_l, got_l)
            side = way if k == chunks - 1 else 1 - way
            total = chip_sum(k + 1, pl.ds(side * part, part))
            if k not in (chunks - 1, chunks - 3):
                before = chunks - 1 if k == chunks - 2 else k + 2
                rs_copy(way, before).wait_recv()
                total = total + got[before].astype(jnp.float32)
            put[k] = total.astype(jnp.bfloat16)
            rs_copy(way, k).start()

    def arrive(slot):
        if slot == 0:
            own_copy(other).wait_recv()
        else:
            for way in range(2):
                pass_copy(way, slot - 1, other).wait_recv()

    ff_tile = ff // 4
    out_tile = width // 4

    def hidden_part(slot, first, last):
        def body(j, carry):
            x = xs[slot].reshape(2 * tok_rows, width)
            cols = pl.ds(pl.multiple_of(j * ff_tile, ff_tile), ff_tile)
            gate = jnp.dot(x, wg[:, cols], preferred_element_type=jnp.float32)
            up = jnp.dot(x, wu[:, cols], preferred_element_type=jnp.float32)
            hid[:, cols] = (gate / (1.0 + jnp.exp(-gate)) * up).astype(jnp.bfloat16)
            return carry

        lax.fori_loop(first, last, body, 0)

    def answer_part(slot):
        def body(j, carry):
            cols = pl.ds(pl.multiple_of(j * out_tile, out_tile), out_tile)
            answer = jnp.dot(hid[...], wd[:, cols], preferred_element_type=jnp.float32)
            scale = jnp.concatenate([gate_col[...]] * (out_tile // 128), axis=1)
            ps[slot, :, :, cols] = (
                (answer * scale).astype(jnp.bfloat16).reshape(2, tok_rows, out_tile)
            )
            return carry

        lax.fori_loop(0, 4, body, 0)

    order = [0] + [k + 1 for k in range(chunks - 4)]
    order += [chunks - 2, chunks, chunks - 1, chunks - 3]
    last = 3 * ring
    hooks = {}
    for k in range(chunks):
        due = min(3 * order.index(later + 1) - 1 for later in range(k, chunks))
        hooks.setdefault(min(due, 5 * k // 2 + 1), []).append(
            functools.partial(ag_event, k)
        )
    firsts, seconds = list(range(chunks - 3, -1, -2)), [chunks - 1]
    seconds += list(range(chunks - 2, 0, -2))
    sends = [k for pair in zip(firsts, seconds) for k in pair] + seconds[len(firsts) :]
    for third, k in zip((last - 10, last - 6, last - 5, last - 2), sends):
        hooks.setdefault(third, []).append(functools.partial(rs_event, k))

    def wait_gate(step, carry):
        gate_copy(step).wait_recv()
        return carry

    third = 0
    for index, slot in enumerate(order):
        arrive(slot)
        if index == 0:
            weight_loads[0].wait()
            weight_loads[1].wait()
        for piece in range(3):
            if piece == 0:
                hidden_part(slot, 0, 2)
            elif piece == 1:
                hidden_part(slot, 2, 4)
            else:
                if index == 0:
                    weight_loads[2].wait()
                    lax.fori_loop(1, n, wait_gate, 0)
                for way in range(2):
                    hop = (slot + 1) // 2
                    lane = (slot + 1 + way) % 2 if slot > 0 else way
                    where = place - hop if way == 0 else place + hop
                    spot = chip_at((where + ring) % ring, ring) * 2
                    for whose in range(2):
                        row = gate_all[(me + n - spot - whose) % n]
                        gate_col[pl.ds(whose * tok_rows + way * part, part), :] = (
                            jnp.broadcast_to(row, (128, tok_rows)).T[
                                lane * part : (lane + 1) * part
                            ]
                        )
                answer_part(slot)
                sib_copy(slot, other).start()
            for hook in hooks.get(third, []):
                hook()
            third += 1

    for k in sends[4:]:
        rs_event(k)
    sib_copy(0, core).wait_recv()
    for lane in (1, 0):
        rows = pl.ds(lane * part, part)
        total = chip_sum(0, rows)
        for way, got in ((0, got_r), (1, got_l)):
            k = 1 if lane == way else 0
            rs_copy(way, k).wait_recv()
            total = total + got[k].astype(jnp.float32)
        out_ref[rows, :] = total.astype(jnp.bfloat16)
    for s in range(chunks):
        for way in range(2):
            ag_copy(way, s).wait_send()
            pass_copy(way, s, core).wait_send()
            rs_copy(way, s).wait_send()
    for slot in range(ring):
        sib_copy(slot, other).wait_send()
    own_copy(core).wait_send()

    def drain_gate(step, carry):
        gate_copy(step).wait_send()
        return carry

    lax.fori_loop(1, n, drain_gate, 0)


def fused_scratch(n, tok_rows, width, ff):
    ring = n // 2
    chunks, part, bf16 = ring - 1, tok_rows // 2, jnp.bfloat16
    buffers = [
        ((ring, 2, tok_rows, width), bf16),
        ((width, ff), bf16),
        ((width, ff), bf16),
        ((ff, width), bf16),
        ((ring, 2, tok_rows, width), bf16),
        ((ring, tok_rows, width), bf16),
        ((chunks, part, width), bf16),
        ((chunks, part, width), bf16),
        ((chunks, part, width), bf16),
        ((chunks, part, width), bf16),
        ((2 * tok_rows, ff), bf16),
        ((n, 1, tok_rows), jnp.float32),
        ((n, 1, tok_rows), jnp.float32),
        ((2 * tok_rows, 128), jnp.float32),
    ]
    sems = [(4,), (n,), (n,), (2, chunks), (2, chunks), (2, chunks), (2, chunks), (2,), (ring,), (ring,), (2, chunks), (2, chunks)]
    size = 0
    for shape, kind in buffers:
        count = jnp.dtype(kind).itemsize
        for extent in shape:
            count = count * extent
        size = size + count
    scratch = [pltpu.VMEM(shape, kind) for shape, kind in buffers]
    return scratch + [pltpu.SemaphoreType.DMA(shape) for shape in sems], size


def fused_device(tokens, expert_ids, route_logits, w_gate, w_up, w_down):
    n = lax.axis_size("ep")
    tok_rows, width = tokens.shape
    ff = w_gate.shape[2]
    scratch, size = fused_scratch(n, tok_rows, width, ff)
    anywhere, vmem = pl.BlockSpec(memory_space=pl.ANY), pl.BlockSpec(memory_space=pltpu.VMEM)
    return pl.pallas_call(
        functools.partial(fused_kernel, n),
        out_shape=jax.ShapeDtypeStruct((tok_rows, width), jnp.bfloat16),
        in_specs=[anywhere, vmem, vmem, anywhere, anywhere, anywhere],
        out_specs=vmem,
        scratch_shapes=scratch,
        compiler_params=pltpu.CompilerParams(
            collective_id=0, has_side_effects=True, vmem_limit_bytes=VMEM_BYTES
        ),
    )(tokens, expert_ids.T, route_logits.T, w_gate, w_up, w_down)


def layer(tokens, expert_ids, route_logits, w_gate, w_up, w_down):
    n = lax.axis_size("ep")
    tok_rows, width = tokens.shape
    ff = w_gate.shape[2]
    size = fused_scratch(n, tok_rows, width, ff)[1]
    fits = size + 8 * tok_rows * width < VMEM_BYTES
    if fits and n % 4 == 0 and n >= 16 and tok_rows == 128 and n <= 128:
        return fused_device(tokens, expert_ids, route_logits, w_gate, w_up, w_down)
    return per_device(tokens, expert_ids, route_logits, w_gate, w_up, w_down)


def solution(mesh):
    in_specs = (
        P(("dp", "ep"), None),
        P(("dp", "ep"), None),
        P(("dp", "ep"), None),
        P("ep", None, None),
        P("ep", None, None),
        P("ep", None, None),
    )
    out_specs = P(("dp", "ep"), None)
    return jax.shard_map(
        layer, mesh=mesh, in_specs=in_specs, out_specs=out_specs, check_vma=False
    )
```

```python
import functools

import jax
import jax.numpy as jnp
from jax import lax
from jax.experimental import pallas as pl
from jax.experimental.pallas import tpu as pltpu
from jax.sharding import PartitionSpec as P

VMEM_BYTES = 63 * 1024 * 1024


def expert_ffn(rows, gate_weight, up_weight, down_weight):
    gate = jnp.dot(rows, gate_weight, preferred_element_type=jnp.float32)
    up_part = jnp.dot(rows, up_weight, preferred_element_type=jnp.float32)
    hidden = (jax.nn.silu(gate) * up_part).astype(jnp.bfloat16)
    return jnp.dot(hidden, down_weight, preferred_element_type=jnp.float32).astype(jnp.bfloat16)


def blockwise(rows, live_rows, weights):
    turns = (live_rows + 127) // 128

    def step(block_index, result):
        first_row = block_index * 128
        block_rows = lax.dynamic_slice_in_dim(rows, first_row, 128, 0)
        answer = expert_ffn(block_rows, weights[0], weights[1], weights[2])
        return lax.dynamic_update_slice_in_dim(result, answer, first_row, 0)

    return lax.fori_loop(jnp.int32(0), turns, step, jnp.zeros(rows.shape, jnp.bfloat16))


def per_device(tokens, expert_ids, route_logits, w_gate, w_up, w_down):
    tok_rows, model_width = tokens.shape
    picks = expert_ids.shape[1]
    experts = lax.axis_size("ep")
    capacity = min(tok_rows, 3 * tok_rows * picks // (2 * experts))
    row_quota = tok_rows * picks
    received = experts * capacity
    spill_count = (max(received - row_quota, 128) + 127) // 128 * 128
    length = row_quota + spill_count
    flat_ids = expert_ids.reshape(-1)
    one_hot = (flat_ids[:, None] == jnp.arange(experts, dtype=jnp.int32)[None, :]).astype(jnp.int32)
    earlier = jnp.cumsum(one_hot, axis=0) - one_hot
    slot_rank = jnp.sum(earlier * one_hot, axis=1)
    counts = jnp.sum(one_hot, axis=0)
    slot_place = flat_ids * capacity + slot_rank
    source_row = jnp.arange(row_quota, dtype=jnp.int32) // picks
    slot_token = jnp.full((received,), tok_rows, jnp.int32).at[slot_place].set(source_row)
    padded_tokens = jnp.concatenate([tokens, jnp.zeros((1, model_width), tokens.dtype)], 0)
    outgoing = padded_tokens[slot_token].reshape(experts, capacity, model_width)
    all_counts = lax.all_gather(counts, "ep", axis=0, tiled=True).reshape(experts, experts)
    own_index = lax.axis_index("ep")
    from_sources = lax.dynamic_index_in_dim(all_counts, own_index, 1, keepdims=False)
    incoming = lax.all_to_all(outgoing, "ep", split_axis=0, concat_axis=0, tiled=True)
    offsets = jnp.cumsum(from_sources) - from_sources
    live_rows = jnp.sum(from_sources)
    slot_numbers = jnp.arange(capacity, dtype=jnp.int32)
    live_slot = slot_numbers[None, :] < from_sources[:, None]
    position = jnp.where(live_slot, offsets[:, None] + slot_numbers[None, :], length).reshape(-1)
    gather_order = (
        jnp.full((length,), received, jnp.int32)
        .at[position]
        .set(jnp.arange(received, dtype=jnp.int32), mode="drop")
    )
    flat_incoming = jnp.concatenate(
        [incoming.reshape(received, model_width), jnp.zeros((1, model_width), jnp.bfloat16)], 0
    )
    packed = flat_incoming[gather_order]
    own_weights = (w_gate[0], w_up[0], w_down[0])
    results = blockwise(packed, live_rows, own_weights)
    results_ext = jnp.concatenate([results, jnp.zeros((1, model_width), jnp.bfloat16)], 0)
    outgoing_back = results_ext[position].reshape(experts, capacity, model_width)
    answers = lax.all_to_all(outgoing_back, "ep", split_axis=0, concat_axis=0, tiled=True)
    mix_weights = jax.nn.softmax(route_logits, axis=-1)
    picked = answers.reshape(received, model_width)[slot_place].reshape(
        tok_rows, picks, model_width
    )
    mixed_rows = jnp.zeros((tok_rows, model_width), jnp.float32)
    for column in range(picks):
        mixed_rows = mixed_rows + mix_weights[:, column : column + 1] * picked[:, column].astype(
            jnp.float32
        )
    return mixed_rows.astype(jnp.bfloat16)


def ring_place(chip, ring):
    column, row = chip % 2, chip // 2
    return row + column * (ring - 1 - 2 * row)


def chip_at(place, ring):
    column = place // (ring // 2)
    return 2 * (place + column * (ring - 1 - 2 * place)) + column


def remote(src, dst, send_sem, recv_sem, target):
    return pltpu.make_async_remote_copy(
        src_ref=src,
        dst_ref=dst,
        send_sem=send_sem,
        recv_sem=recv_sem,
        device_id={"ep": target},
        device_id_type=pl.DeviceIdType.MESH,
    )


def fused_kernel(
    n,
    tok_ref,
    ids_ref,
    logits_ref,
    wg_hbm,
    wu_hbm,
    wd_hbm,
    out_ref,
    xs,
    wg,
    wu,
    wd,
    ps,
    sib,
    got_r,
    got_l,
    put_r,
    put_l,
    hid,
    gate_rows,
    gate_all,
    gate_col,
    load_sem,
    gate_send,
    gate_recv,
    gate_out,
    gate_in,
    ag_send,
    ag_recv,
    pass_send,
    pass_recv,
    own_sem,
    sib_send,
    sib_recv,
    rs_send,
    rs_recv,
):
    ring = n // 2
    far = ring // 2
    chunks = ring - 1
    tok_rows, width = tok_ref.shape
    part = tok_rows // 2
    ff = wg.shape[1]
    me = lax.axis_index("ep")
    core, chip = me % 2, me // 2
    other = 1 - core
    place = ring_place(chip, ring)
    right = chip_at((place + 1) % ring, ring) * 2 + core
    left = chip_at((place + ring - 1) % ring, ring) * 2 + core
    twin = chip * 2 + other

    barrier = pltpu.get_barrier_semaphore()

    for friend in (right, left, twin):
        pl.semaphore_signal(
            barrier,
            inc=1,
            device_id={"ep": friend},
            device_id_type=pl.DeviceIdType.MESH,
        )

    own_load = pltpu.make_async_copy(tok_ref, xs.at[0, core], load_sem.at[0])
    own_load.start()
    weight_loads = [
        pltpu.make_async_copy(wg_hbm.at[0], wg, load_sem.at[1]),
        pltpu.make_async_copy(wu_hbm.at[0], wu, load_sem.at[2]),
        pltpu.make_async_copy(wd_hbm.at[0], wd, load_sem.at[3]),
    ]
    for load in weight_loads:
        load.start()

    logits = logits_ref[...]
    powers = jnp.exp(logits - jnp.max(logits, axis=0, keepdims=True))
    gates = powers / jnp.sum(powers, axis=0, keepdims=True)
    ids = ids_ref[...]
    for expert in range(n):
        gate_rows[core, expert] = jnp.sum(
            jnp.where(ids == expert, gates, 0.0), axis=0, keepdims=True
        )

    own_load.wait()
    pl.semaphore_wait(barrier, 3)

    def ag_copy(way, s):
        target = right if way == 0 else left
        rows = pl.ds(way * part, part)
        if s < 2:
            lane = s if way == 0 else 1 - s
            src = xs.at[0, core, pl.ds(lane * part, part)]
        else:
            src = xs.at[s - 1, core, rows]
        return remote(
            src, xs.at[s + 1, core, rows], ag_send.at[way, s], ag_recv.at[way, s], target
        )

    def pass_copy(way, s, whose):
        ref = xs.at[s + 1, whose, pl.ds(way * part, part)]
        return remote(ref, ref, pass_send.at[way, s], pass_recv.at[way, s], twin)

    def own_copy(whose):
        ref = xs.at[0, whose]
        return remote(ref, ref, own_sem.at[0], own_sem.at[1], twin)

    def own_gate(whose):
        ref = gate_rows.at[whose]
        return remote(ref, ref, own_sem.at[2], own_sem.at[3], twin)

    def gate_copy(way, hop):
        return remote(
            gate_rows.at[core] if hop == 1 else gate_all.at[way, hop - 2, core],
            gate_all.at[way, hop - 1, core],
            gate_send.at[way, hop - 1],
            gate_recv.at[way, hop - 1],
            right if way == 0 else left,
        )

    def gate_pass(way, hop, whose):
        ref = gate_all.at[way, hop - 1, whose]
        return remote(
            ref, ref, gate_out.at[way, hop - 1], gate_in.at[way, hop - 1], twin
        )

    for way in range(2):
        ag_copy(way, 0).start()
    for way in range(2):
        ag_copy(way, 1).start()
        gate_copy(way, 1).start()
    own_copy(core).start()
    own_gate(core).start()

    turns = list(range(chunks - 4)) + [chunks - 3, chunks - 4, chunks - 1, chunks - 2]
    waiting, seen = [s for s in turns if s >= 2], set()

    def ag_event(k):
        seen.add(k)
        ready = []
        while waiting and waiting[0] - 2 in seen:
            ready.append(waiting.pop(0))
        for way in range(2):
            ag_copy(way, k).wait_recv()
            for s in ready:
                ag_copy(way, s).start()
            pass_copy(way, k, core).start()
            if k % 2 == 0:
                hop = k // 2 + 1
                gate_copy(way, hop).wait_recv()
                if hop < far:
                    gate_copy(way, hop + 1).start()
                gate_pass(way, hop, core).start()

    def sib_copy(slot, whose):
        return remote(
            ps.at[slot, whose], sib.at[slot], sib_send.at[slot], sib_recv.at[slot], twin
        )

    def rs_copy(way, k):
        put, got, target = (put_r, got_r, right) if way == 0 else (put_l, got_l, left)
        return remote(
            put.at[k], got.at[k], rs_send.at[way, k], rs_recv.at[way, k], target
        )

    def chip_sum(slot, rows):
        return ps[slot, core, rows, :].astype(jnp.float32) + sib[slot, rows, :].astype(
            jnp.float32
        )

    def rs_event(k):
        sib_copy(k + 1, core).wait_recv()
        for way in range(2):
            put, got = (put_r, got_r) if way == 0 else (put_l, got_l)
            side = way if k == chunks - 1 else 1 - way
            total = chip_sum(k + 1, pl.ds(side * part, part))
            if k not in (chunks - 1, chunks - 3):
                before = chunks - 1 if k == chunks - 2 else k + 2
                rs_copy(way, before).wait_recv()
                total = total + got[before].astype(jnp.float32)
            put[k] = total.astype(jnp.bfloat16)
            rs_copy(way, k).start()

    def arrive(slot):
        if slot == 0:
            own_copy(other).wait_recv()
            own_gate(other).wait_recv()
        else:
            for way in range(2):
                pass_copy(way, slot - 1, other).wait_recv()
                if slot % 2 == 1:
                    gate_pass(way, (slot + 1) // 2, other).wait_recv()

    ff_tile = ff // 4
    out_tile = width // 4

    def hidden_part(slot, first, last):
        def body(j, carry):
            x = xs[slot].reshape(2 * tok_rows, width)
            cols = pl.ds(pl.multiple_of(j * ff_tile, ff_tile), ff_tile)
            gate = jnp.dot(x, wg[:, cols], preferred_element_type=jnp.float32)
            up = jnp.dot(x, wu[:, cols], preferred_element_type=jnp.float32)
            hid[:, cols] = (gate / (1.0 + jnp.exp(-gate)) * up).astype(jnp.bfloat16)
            return carry

        lax.fori_loop(first, last, body, 0)

    def answer_part(slot):
        def body(j, carry):
            cols = pl.ds(pl.multiple_of(j * out_tile, out_tile), out_tile)
            answer = jnp.dot(hid[...], wd[:, cols], preferred_element_type=jnp.float32)
            scale = jnp.concatenate([gate_col[...]] * (out_tile // 128), axis=1)
            ps[slot, :, :, cols] = (
                (answer * scale).astype(jnp.bfloat16).reshape(2, tok_rows, out_tile)
            )
            return carry

        lax.fori_loop(0, 4, body, 0)

    order = [0] + [k + 1 for k in range(chunks - 4)]
    order += [chunks - 2, chunks, chunks - 1, chunks - 3]
    last = 3 * ring
    hooks = {}
    times = [(5 * i + 1) // 2 + 1 for i in range(chunks - 4)]
    times += [last - 14, last - 12, last - 10, last - 7]
    for time, k in zip(times, turns):
        hooks.setdefault(time, []).append(functools.partial(ag_event, k))
    firsts, seconds = list(range(chunks - 3, -1, -2)), [chunks - 1]
    seconds += list(range(chunks - 2, 0, -2))
    sends = [k for pair in zip(firsts, seconds) for k in pair] + seconds[len(firsts) :]
    for third, k in zip((last - 10, last - 6, last - 5, last - 2), sends):
        hooks.setdefault(third, []).append(functools.partial(rs_event, k))

    third = 0
    for index, slot in enumerate(order):
        arrive(slot)
        if index == 0:
            weight_loads[0].wait()
            weight_loads[1].wait()
        for piece in range(3):
            if piece == 0:
                hidden_part(slot, 0, 2)
            elif piece == 1:
                hidden_part(slot, 2, 4)
            else:
                if index == 0:
                    weight_loads[2].wait()
                for way in range(2):
                    hop = (slot + 1) // 2
                    lane = (slot + 1 + way) % 2 if slot > 0 else way
                    for whose in range(2):
                        if hop == 0:
                            row = gate_rows[whose, me]
                        else:
                            row = gate_all[way, hop - 1, whose, me]
                        gate_col[pl.ds(whose * tok_rows + way * part, part), :] = (
                            jnp.broadcast_to(row, (128, tok_rows)).T[
                                lane * part : (lane + 1) * part
                            ]
                        )
                answer_part(slot)
                sib_copy(slot, other).start()
            for hook in hooks.get(third, []):
                hook()
            third += 1

    for k in sends[4:]:
        rs_event(k)
    sib_copy(0, core).wait_recv()
    for lane in (1, 0):
        rows = pl.ds(lane * part, part)
        total = chip_sum(0, rows)
        for way, got in ((0, got_r), (1, got_l)):
            k = 1 if lane == way else 0
            rs_copy(way, k).wait_recv()
            total = total + got[k].astype(jnp.float32)
        out_ref[rows, :] = total.astype(jnp.bfloat16)
    for s in range(chunks):
        for way in range(2):
            ag_copy(way, s).wait_send()
            pass_copy(way, s, core).wait_send()
            rs_copy(way, s).wait_send()
    for slot in range(ring):
        sib_copy(slot, other).wait_send()
    own_copy(core).wait_send()
    own_gate(core).wait_send()
    for hop in range(1, far + 1):
        for way in range(2):
            gate_copy(way, hop).wait_send()
            gate_pass(way, hop, core).wait_send()


def fused_scratch(n, tok_rows, width, ff):
    ring = n // 2
    chunks, part, bf16 = ring - 1, tok_rows // 2, jnp.bfloat16
    buffers = [
        ((ring, 2, tok_rows, width), bf16),
        ((width, ff), bf16),
        ((width, ff), bf16),
        ((ff, width), bf16),
        ((ring, 2, tok_rows, width), bf16),
        ((ring, tok_rows, width), bf16),
        ((chunks, part, width), bf16),
        ((chunks, part, width), bf16),
        ((chunks, part, width), bf16),
        ((chunks, part, width), bf16),
        ((2 * tok_rows, ff), bf16),
        ((2, n, 1, tok_rows), jnp.float32),
        ((2, ring // 2, 2, n, 1, tok_rows), jnp.float32),
        ((2 * tok_rows, 128), jnp.float32),
    ]
    hops, moves = (2, ring // 2), (2, chunks)
    sems = [(4,), hops, hops, hops, hops, moves, moves, moves, moves, (4,)]
    sems += [(ring,), (ring,), moves, moves]
    size = 0
    for shape, kind in buffers:
        count = jnp.dtype(kind).itemsize
        for extent in shape:
            count = count * extent
        size = size + count
    scratch = [pltpu.VMEM(shape, kind) for shape, kind in buffers]
    return scratch + [pltpu.SemaphoreType.DMA(shape) for shape in sems], size


def fused_device(tokens, expert_ids, route_logits, w_gate, w_up, w_down):
    n = lax.axis_size("ep")
    tok_rows, width = tokens.shape
    ff = w_gate.shape[2]
    scratch, size = fused_scratch(n, tok_rows, width, ff)
    anywhere, vmem = pl.BlockSpec(memory_space=pl.ANY), pl.BlockSpec(memory_space=pltpu.VMEM)
    return pl.pallas_call(
        functools.partial(fused_kernel, n),
        out_shape=jax.ShapeDtypeStruct((tok_rows, width), jnp.bfloat16),
        in_specs=[anywhere, vmem, vmem, anywhere, anywhere, anywhere],
        out_specs=vmem,
        scratch_shapes=scratch,
        compiler_params=pltpu.CompilerParams(
            collective_id=0, has_side_effects=True, vmem_limit_bytes=VMEM_BYTES
        ),
    )(tokens, expert_ids.T, route_logits.T, w_gate, w_up, w_down)


def layer(tokens, expert_ids, route_logits, w_gate, w_up, w_down):
    n = lax.axis_size("ep")
    tok_rows, width = tokens.shape
    ff = w_gate.shape[2]
    size = fused_scratch(n, tok_rows, width, ff)[1]
    fits = size + 8 * tok_rows * width < VMEM_BYTES
    if fits and n % 4 == 0 and n >= 16 and tok_rows == 128 and n <= 128:
        return fused_device(tokens, expert_ids, route_logits, w_gate, w_up, w_down)
    return per_device(tokens, expert_ids, route_logits, w_gate, w_up, w_down)


def solution(mesh):
    in_specs = (
        P(("dp", "ep"), None),
        P(("dp", "ep"), None),
        P(("dp", "ep"), None),
        P("ep", None, None),
        P("ep", None, None),
        P("ep", None, None),
    )
    out_specs = P(("dp", "ep"), None)
    return jax.shard_map(
        layer, mesh=mesh, in_specs=in_specs, out_specs=out_specs, check_vma=False
    )
```

```python
import functools

import jax
import jax.numpy as jnp
from jax import lax
from jax.experimental import pallas as pl
from jax.experimental.pallas import tpu as pltpu
from jax.sharding import PartitionSpec as P

VMEM_BYTES = 63 * 1024 * 1024


def expert_ffn(rows, gate_weight, up_weight, down_weight):
    gate = jnp.dot(rows, gate_weight, preferred_element_type=jnp.float32)
    up_part = jnp.dot(rows, up_weight, preferred_element_type=jnp.float32)
    hidden = (jax.nn.silu(gate) * up_part).astype(jnp.bfloat16)
    return jnp.dot(hidden, down_weight, preferred_element_type=jnp.float32).astype(jnp.bfloat16)


def blockwise(rows, live_rows, weights):
    turns = (live_rows + 127) // 128

    def step(block_index, result):
        first_row = block_index * 128
        block_rows = lax.dynamic_slice_in_dim(rows, first_row, 128, 0)
        answer = expert_ffn(block_rows, weights[0], weights[1], weights[2])
        return lax.dynamic_update_slice_in_dim(result, answer, first_row, 0)

    return lax.fori_loop(jnp.int32(0), turns, step, jnp.zeros(rows.shape, jnp.bfloat16))


def per_device(tokens, expert_ids, route_logits, w_gate, w_up, w_down):
    tok_rows, model_width = tokens.shape
    picks = expert_ids.shape[1]
    experts = lax.axis_size("ep")
    capacity = min(tok_rows, 3 * tok_rows * picks // (2 * experts))
    row_quota = tok_rows * picks
    received = experts * capacity
    spill_count = (max(received - row_quota, 128) + 127) // 128 * 128
    length = row_quota + spill_count
    flat_ids = expert_ids.reshape(-1)
    one_hot = (flat_ids[:, None] == jnp.arange(experts, dtype=jnp.int32)[None, :]).astype(jnp.int32)
    earlier = jnp.cumsum(one_hot, axis=0) - one_hot
    slot_rank = jnp.sum(earlier * one_hot, axis=1)
    counts = jnp.sum(one_hot, axis=0)
    slot_place = flat_ids * capacity + slot_rank
    source_row = jnp.arange(row_quota, dtype=jnp.int32) // picks
    slot_token = jnp.full((received,), tok_rows, jnp.int32).at[slot_place].set(source_row)
    padded_tokens = jnp.concatenate([tokens, jnp.zeros((1, model_width), tokens.dtype)], 0)
    outgoing = padded_tokens[slot_token].reshape(experts, capacity, model_width)
    all_counts = lax.all_gather(counts, "ep", axis=0, tiled=True).reshape(experts, experts)
    own_index = lax.axis_index("ep")
    from_sources = lax.dynamic_index_in_dim(all_counts, own_index, 1, keepdims=False)
    incoming = lax.all_to_all(outgoing, "ep", split_axis=0, concat_axis=0, tiled=True)
    offsets = jnp.cumsum(from_sources) - from_sources
    live_rows = jnp.sum(from_sources)
    slot_numbers = jnp.arange(capacity, dtype=jnp.int32)
    live_slot = slot_numbers[None, :] < from_sources[:, None]
    position = jnp.where(live_slot, offsets[:, None] + slot_numbers[None, :], length).reshape(-1)
    gather_order = (
        jnp.full((length,), received, jnp.int32)
        .at[position]
        .set(jnp.arange(received, dtype=jnp.int32), mode="drop")
    )
    flat_incoming = jnp.concatenate(
        [incoming.reshape(received, model_width), jnp.zeros((1, model_width), jnp.bfloat16)], 0
    )
    packed = flat_incoming[gather_order]
    own_weights = (w_gate[0], w_up[0], w_down[0])
    results = blockwise(packed, live_rows, own_weights)
    results_ext = jnp.concatenate([results, jnp.zeros((1, model_width), jnp.bfloat16)], 0)
    outgoing_back = results_ext[position].reshape(experts, capacity, model_width)
    answers = lax.all_to_all(outgoing_back, "ep", split_axis=0, concat_axis=0, tiled=True)
    mix_weights = jax.nn.softmax(route_logits, axis=-1)
    picked = answers.reshape(received, model_width)[slot_place].reshape(
        tok_rows, picks, model_width
    )
    mixed_rows = jnp.zeros((tok_rows, model_width), jnp.float32)
    for column in range(picks):
        mixed_rows = mixed_rows + mix_weights[:, column : column + 1] * picked[:, column].astype(
            jnp.float32
        )
    return mixed_rows.astype(jnp.bfloat16)


def ring_place(chip, ring):
    column, row = chip % 2, chip // 2
    return row + column * (ring - 1 - 2 * row)


def chip_at(place, ring):
    column = place // (ring // 2)
    return 2 * (place + column * (ring - 1 - 2 * place)) + column


def remote(src, dst, send_sem, recv_sem, target):
    return pltpu.make_async_remote_copy(
        src_ref=src,
        dst_ref=dst,
        send_sem=send_sem,
        recv_sem=recv_sem,
        device_id={"ep": target},
        device_id_type=pl.DeviceIdType.MESH,
    )


def fused_kernel(
    n,
    tok_ref,
    ids_ref,
    logits_ref,
    wg_hbm,
    wu_hbm,
    wd_hbm,
    out_ref,
    xs,
    wg,
    wu,
    wd,
    ps,
    sib,
    got_r,
    got_l,
    put_r,
    put_l,
    hid,
    gate_rows,
    gate_all,
    gate_col,
    load_sem,
    gate_send,
    gate_recv,
    gate_out,
    gate_in,
    ag_send,
    ag_recv,
    pass_send,
    pass_recv,
    own_sem,
    sib_send,
    sib_recv,
    rs_send,
    rs_recv,
):
    ring = n // 2
    far = ring // 2
    chunks = ring - 1
    tok_rows, width = tok_ref.shape
    part = tok_rows // 2
    ff = wg.shape[1]
    me = lax.axis_index("ep")
    core, chip = me % 2, me // 2
    other = 1 - core
    place = ring_place(chip, ring)
    right = chip_at((place + 1) % ring, ring) * 2 + core
    left = chip_at((place + ring - 1) % ring, ring) * 2 + core
    twin = chip * 2 + other

    barrier = pltpu.get_barrier_semaphore()

    for friend in (right, left, twin):
        pl.semaphore_signal(
            barrier,
            inc=1,
            device_id={"ep": friend},
            device_id_type=pl.DeviceIdType.MESH,
        )

    own_load = pltpu.make_async_copy(tok_ref, xs.at[0, core], load_sem.at[0])
    own_load.start()
    weight_loads = [
        pltpu.make_async_copy(wg_hbm.at[0], wg, load_sem.at[1]),
        pltpu.make_async_copy(wu_hbm.at[0], wu, load_sem.at[2]),
        pltpu.make_async_copy(wd_hbm.at[0], wd, load_sem.at[3]),
    ]
    for load in weight_loads:
        load.start()

    logits = logits_ref[...]
    powers = jnp.exp(logits - jnp.max(logits, axis=0, keepdims=True))
    gates = powers / jnp.sum(powers, axis=0, keepdims=True)
    ids = ids_ref[...]
    for expert in range(n):
        gate_rows[core, expert] = jnp.sum(
            jnp.where(ids == expert, gates, 0.0), axis=0, keepdims=True
        )

    own_load.wait()
    pl.semaphore_wait(barrier, 3)

    def ag_copy(way, s):
        target = right if way == 0 else left
        rows = pl.ds(way * part, part)
        if s < 2:
            lane = s if way == 0 else 1 - s
            src = xs.at[0, core, pl.ds(lane * part, part)]
        else:
            src = xs.at[s - 1, core, rows]
        return remote(
            src, xs.at[s + 1, core, rows], ag_send.at[way, s], ag_recv.at[way, s], target
        )

    def pass_copy(way, s, whose):
        ref = xs.at[s + 1, whose, pl.ds(way * part, part)]
        return remote(ref, ref, pass_send.at[way, s], pass_recv.at[way, s], twin)

    def own_copy(whose):
        ref = xs.at[0, whose]
        return remote(ref, ref, own_sem.at[0], own_sem.at[1], twin)

    def own_gate(whose):
        ref = gate_rows.at[whose]
        return remote(ref, ref, own_sem.at[2], own_sem.at[3], twin)

    def gate_copy(way, hop):
        return remote(
            gate_rows.at[core] if hop == 1 else gate_all.at[way, hop - 2, core],
            gate_all.at[way, hop - 1, core],
            gate_send.at[way, hop - 1],
            gate_recv.at[way, hop - 1],
            right if way == 0 else left,
        )

    def gate_pass(way, hop, whose):
        ref = gate_all.at[way, hop - 1, whose]
        return remote(
            ref, ref, gate_out.at[way, hop - 1], gate_in.at[way, hop - 1], twin
        )

    for way in range(2):
        gate_copy(way, 1).start()
        ag_copy(way, 0).start()
    for way in range(2):
        ag_copy(way, 1).start()
    own_copy(core).start()
    own_gate(core).start()

    turns = list(range(chunks - 4)) + [chunks - 3, chunks - 4, chunks - 1, chunks - 2]
    waiting, seen = [s for s in turns if s >= 2], set()

    def ag_event(k):
        seen.add(k)
        ready = []
        while waiting and waiting[0] - 2 in seen:
            ready.append(waiting.pop(0))
        for way in range(2):
            hop = k // 2 + 1
            if k % 2 == 0:
                gate_copy(way, hop).wait_recv()
                if hop < far:
                    gate_copy(way, hop + 1).start()
            ag_copy(way, k).wait_recv()
            for s in ready:
                ag_copy(way, s).start()
            pass_copy(way, k, core).start()
            if k % 2 == 0:
                gate_pass(way, hop, core).start()

    def sib_copy(slot, whose):
        return remote(
            ps.at[slot, whose], sib.at[slot], sib_send.at[slot], sib_recv.at[slot], twin
        )

    def rs_copy(way, k):
        put, got, target = (put_r, got_r, right) if way == 0 else (put_l, got_l, left)
        return remote(
            put.at[k], got.at[k], rs_send.at[way, k], rs_recv.at[way, k], target
        )

    def chip_sum(slot, rows):
        return ps[slot, core, rows, :].astype(jnp.float32) + sib[slot, rows, :].astype(
            jnp.float32
        )

    def rs_event(k):
        sib_copy(k + 1, core).wait_recv()
        for way in range(2):
            put, got = (put_r, got_r) if way == 0 else (put_l, got_l)
            side = way if k == chunks - 1 else 1 - way
            total = chip_sum(k + 1, pl.ds(side * part, part))
            if k not in (chunks - 1, chunks - 3):
                before = chunks - 1 if k == chunks - 2 else k + 2
                rs_copy(way, before).wait_recv()
                total = total + got[before].astype(jnp.float32)
            put[k] = total.astype(jnp.bfloat16)
            rs_copy(way, k).start()

    def arrive(slot):
        if slot == 0:
            own_copy(other).wait_recv()
            own_gate(other).wait_recv()
        else:
            for way in range(2):
                pass_copy(way, slot - 1, other).wait_recv()
                if slot % 2 == 1:
                    gate_pass(way, (slot + 1) // 2, other).wait_recv()

    ff_tile = ff // 4
    out_tile = width // 4

    def hidden_part(slot, first, last):
        def body(j, carry):
            x = xs[slot].reshape(2 * tok_rows, width)
            cols = pl.ds(pl.multiple_of(j * ff_tile, ff_tile), ff_tile)
            gate = jnp.dot(x, wg[:, cols], preferred_element_type=jnp.float32)
            up = jnp.dot(x, wu[:, cols], preferred_element_type=jnp.float32)
            hid[:, cols] = (gate / (1.0 + jnp.exp(-gate)) * up).astype(jnp.bfloat16)
            return carry

        lax.fori_loop(first, last, body, 0)

    def answer_part(slot):
        def body(j, carry):
            cols = pl.ds(pl.multiple_of(j * out_tile, out_tile), out_tile)
            answer = jnp.dot(hid[...], wd[:, cols], preferred_element_type=jnp.float32)
            scale = jnp.concatenate([gate_col[...]] * (out_tile // 128), axis=1)
            ps[slot, :, :, cols] = (
                (answer * scale).astype(jnp.bfloat16).reshape(2, tok_rows, out_tile)
            )
            return carry

        lax.fori_loop(0, 4, body, 0)

    order = [0] + [k + 1 for k in range(chunks - 4)]
    order += [chunks - 2, chunks, chunks - 1, chunks - 3]
    last = 3 * ring
    hooks = {}
    times = [(5 * i + 1) // 2 + 1 for i in range(chunks - 4)]
    times += [last - 14, last - 12, last - 10, last - 7]
    for time, k in zip(times, turns):
        hooks.setdefault(time, []).append(functools.partial(ag_event, k))
    firsts, seconds = list(range(chunks - 3, -1, -2)), [chunks - 1]
    seconds += list(range(chunks - 2, 0, -2))
    sends = [k for pair in zip(firsts, seconds) for k in pair] + seconds[len(firsts) :]
    for third, k in zip((last - 10, last - 6, last - 5, last - 2), sends):
        hooks.setdefault(third, []).append(functools.partial(rs_event, k))

    third = 0
    for index, slot in enumerate(order):
        arrive(slot)
        if index == 0:
            weight_loads[0].wait()
            weight_loads[1].wait()
        for piece in range(3):
            if piece == 0:
                hidden_part(slot, 0, 2)
            elif piece == 1:
                hidden_part(slot, 2, 4)
            else:
                if index == 0:
                    weight_loads[2].wait()
                for way in range(2):
                    hop = (slot + 1) // 2
                    lane = (slot + 1 + way) % 2 if slot > 0 else way
                    for whose in range(2):
                        if hop == 0:
                            row = gate_rows[whose, me]
                        else:
                            row = gate_all[way, hop - 1, whose, me]
                        gate_col[pl.ds(whose * tok_rows + way * part, part), :] = (
                            jnp.broadcast_to(row, (128, tok_rows)).T[
                                lane * part : (lane + 1) * part
                            ]
                        )
                answer_part(slot)
                sib_copy(slot, other).start()
            for hook in hooks.get(third, []):
                hook()
            third += 1

    for k in sends[4:]:
        rs_event(k)
    sib_copy(0, core).wait_recv()
    for lane in (1, 0):
        rows = pl.ds(lane * part, part)
        total = chip_sum(0, rows)
        for way, got in ((0, got_r), (1, got_l)):
            k = 1 if lane == way else 0
            rs_copy(way, k).wait_recv()
            total = total + got[k].astype(jnp.float32)
        out_ref[rows, :] = total.astype(jnp.bfloat16)
    for s in range(chunks):
        for way in range(2):
            ag_copy(way, s).wait_send()
            pass_copy(way, s, core).wait_send()
            rs_copy(way, s).wait_send()
    for slot in range(ring):
        sib_copy(slot, other).wait_send()
    own_copy(core).wait_send()
    own_gate(core).wait_send()
    for hop in range(1, far + 1):
        for way in range(2):
            gate_copy(way, hop).wait_send()
            gate_pass(way, hop, core).wait_send()


def fused_scratch(n, tok_rows, width, ff):
    ring = n // 2
    chunks, part, bf16 = ring - 1, tok_rows // 2, jnp.bfloat16
    buffers = [
        ((ring, 2, tok_rows, width), bf16),
        ((width, ff), bf16),
        ((width, ff), bf16),
        ((ff, width), bf16),
        ((ring, 2, tok_rows, width), bf16),
        ((ring, tok_rows, width), bf16),
        ((chunks, part, width), bf16),
        ((chunks, part, width), bf16),
        ((chunks, part, width), bf16),
        ((chunks, part, width), bf16),
        ((2 * tok_rows, ff), bf16),
        ((2, n, 1, tok_rows), jnp.float32),
        ((2, ring // 2, 2, n, 1, tok_rows), jnp.float32),
        ((2 * tok_rows, 128), jnp.float32),
    ]
    hops, moves = (2, ring // 2), (2, chunks)
    sems = [(4,), hops, hops, hops, hops, moves, moves, moves, moves, (4,)]
    sems += [(ring,), (ring,), moves, moves]
    size = 0
    for shape, kind in buffers:
        count = jnp.dtype(kind).itemsize
        for extent in shape:
            count = count * extent
        size = size + count
    scratch = [pltpu.VMEM(shape, kind) for shape, kind in buffers]
    return scratch + [pltpu.SemaphoreType.DMA(shape) for shape in sems], size


def fused_device(tokens, expert_ids, route_logits, w_gate, w_up, w_down):
    n = lax.axis_size("ep")
    tok_rows, width = tokens.shape
    ff = w_gate.shape[2]
    scratch, size = fused_scratch(n, tok_rows, width, ff)
    anywhere, vmem = pl.BlockSpec(memory_space=pl.ANY), pl.BlockSpec(memory_space=pltpu.VMEM)
    return pl.pallas_call(
        functools.partial(fused_kernel, n),
        out_shape=jax.ShapeDtypeStruct((tok_rows, width), jnp.bfloat16),
        in_specs=[anywhere, vmem, vmem, anywhere, anywhere, anywhere],
        out_specs=vmem,
        scratch_shapes=scratch,
        compiler_params=pltpu.CompilerParams(
            collective_id=0, has_side_effects=True, vmem_limit_bytes=VMEM_BYTES
        ),
    )(tokens, expert_ids.T, route_logits.T, w_gate, w_up, w_down)


def layer(tokens, expert_ids, route_logits, w_gate, w_up, w_down):
    n = lax.axis_size("ep")
    tok_rows, width = tokens.shape
    ff = w_gate.shape[2]
    size = fused_scratch(n, tok_rows, width, ff)[1]
    fits = size + 8 * tok_rows * width < VMEM_BYTES
    if fits and n % 4 == 0 and n >= 16 and tok_rows == 128 and n <= 128:
        return fused_device(tokens, expert_ids, route_logits, w_gate, w_up, w_down)
    return per_device(tokens, expert_ids, route_logits, w_gate, w_up, w_down)


def solution(mesh):
    in_specs = (
        P(("dp", "ep"), None),
        P(("dp", "ep"), None),
        P(("dp", "ep"), None),
        P("ep", None, None),
        P("ep", None, None),
        P("ep", None, None),
    )
    out_specs = P(("dp", "ep"), None)
    return jax.shard_map(
        layer, mesh=mesh, in_specs=in_specs, out_specs=out_specs, check_vma=False
    )
```
